256 devices in a mesh: tok: 64 (over z, y, core), unit: 4 (over x).
Axes of the slice: x: 4, y: 4, z: 8, core: 2. Of those that a mesh axis runs over, the one named last changes fastest.
Arguments:
- act_a: bfloat16 [131072, 3072], P('tok', 'unit'), may hold values from -4000 to 4000
- act_b: bfloat16 [131072, 3072], P(('tok', 'unit')), may hold values from -4000 to 4000
Outputs:
- correlation: float32 [3072, 3072], P('tok', 'unit')
The draws below stay inside these ranges and needn't reach their ends.
All inputs are finite; a program needn't handle non-finite values.
Results may differ from the reference program's by a relative error of at most 0.0003.
Values may be sent and summed in bfloat16 or wider, within the bound.
No kernel may reach another device: no remote copies, remote signals or barrier semaphores. Data moves between devices by JAX's collectives and lax.ppermute only.
A program may use at most 128 MiB of HBM per device.

```python
import math
import jax
import jax.numpy as jnp
from jax import lax

U = 3072
TOK_DEV = 2048
TOKENS = 131072
N_TOK = 64


def shared_parts(key):
    latent = jnp.clip(jax.random.normal(jax.random.fold_in(key, 101), (TOKENS, U), jnp.float32), -6.0, 6.0)
    position = jnp.arange(TOKENS, dtype=jnp.float32) / TOKENS
    growth = math.log(3.0)
    jitter = jax.random.uniform(jax.random.fold_in(key, 102), (TOKENS,), jnp.float32, -0.6, 0.6)
    token_scale = jnp.exp(growth * position + jitter)
    return (latent, token_scale)


def own_noise(key):
    return jnp.clip(jax.random.normal(key, (TOKENS, U), jnp.float32), -6.0, 6.0)


def draw_act_a(key, part):
    latent, token_scale = shared_parts(key)
    own_key = jax.random.fold_in(key, 201)
    unit_scale = jnp.exp(jax.random.uniform(jax.random.fold_in(own_key, 1), (U,), jnp.float32, 0.0, math.log(10.0)))
    offset = jnp.clip(jax.random.normal(jax.random.fold_in(own_key, 2), (U,), jnp.float32), -3.0, 3.0)
    noise = own_noise(jax.random.fold_in(own_key, 3))
    value = unit_scale[None, :] * token_scale[:, None] * (offset[None, :] + latent + 0.7 * noise)
    return value.astype(jnp.bfloat16)


def draw_act_b(key, part):
    latent, token_scale = shared_parts(key)
    own_key = jax.random.fold_in(key, 301)
    unit_scale = jnp.exp(jax.random.uniform(jax.random.fold_in(own_key, 1), (U,), jnp.float32, 0.0, math.log(10.0)))
    offset = jnp.clip(jax.random.normal(jax.random.fold_in(own_key, 2), (U,), jnp.float32), -3.0, 3.0)
    noise = own_noise(jax.random.fold_in(own_key, 3))
    order = jax.random.permutation(jax.random.fold_in(own_key, 4), U)
    weight = jax.random.uniform(jax.random.fold_in(own_key, 5), (U,), jnp.float32, -1.2, 1.2)
    moved = jnp.take(latent, order, axis=1)
    value = unit_scale[None, :] * token_scale[:, None] * (offset[None, :] + weight[None, :] * moved + 0.7 * noise)
    return value.astype(jnp.bfloat16)


def setup_inputs(seed: int = 0) -> dict:
    keys = jax.random.split(jax.random.key(seed), 3)
    act_a = draw_act_a(jax.random.fold_in(keys[2], 71), 0)
    act_b = draw_act_b(jax.random.fold_in(keys[2], 71), 0)
    return dict(act_a=act_a, act_b=act_b)


def reference(act_a, act_b):

    def step(carry, index):
        raw, first_total, first_square, second_total, second_square = carry
        start = (index * TOK_DEV).astype(jnp.int32)
        block_a = lax.dynamic_slice_in_dim(act_a, start, TOK_DEV, 0)
        block_b = lax.dynamic_slice_in_dim(act_b, start, TOK_DEV, 0)
        raw = raw + jnp.dot(block_b.T, block_a, preferred_element_type=jnp.float32)
        wide_a = block_a.astype(jnp.float32)
        wide_b = block_b.astype(jnp.float32)
        first_total = first_total + lax.optimization_barrier(jnp.sum(wide_a, axis=0))
        first_square = first_square + lax.optimization_barrier(jnp.sum(wide_a * wide_a, axis=0))
        second_total = second_total + lax.optimization_barrier(jnp.sum(wide_b, axis=0))
        second_square = second_square + lax.optimization_barrier(jnp.sum(wide_b * wide_b, axis=0))
        return ((raw, first_total, first_square, second_total, second_square), None)
    zeros_unit = jnp.zeros((U,), jnp.float32)
    start_carry = (jnp.zeros((U, U), jnp.float32), zeros_unit, zeros_unit, zeros_unit, zeros_unit)
    final, _ = lax.scan(step, start_carry, jnp.arange(N_TOK, dtype=jnp.int32))
    raw, first_total, first_square, second_total, second_square = final
    mean_a = first_total / TOKENS
    var_a = first_square / TOKENS - mean_a * mean_a
    mean_b = second_total / TOKENS
    var_b = second_square / TOKENS - mean_b * mean_b
    centered = raw / TOKENS - mean_b[:, None] * mean_a[None, :]
    return centered / (jnp.sqrt(var_b + 1e-05)[:, None] * jnp.sqrt(var_a + 1e-05)[None, :])
```

```python
import functools

import jax
import jax.numpy as jnp
from jax import lax
from jax.sharding import Mesh
from jax.sharding import PartitionSpec as P

NZ, NY, NC, NX = 8, 4, 2, 4
SIZE = {"z": NZ, "y": NY, "c": NC, "x": NX}
TOK = ("z", "y", "c")
CHUNKS = ((0, 4), (1, 5), (2, 6), (3, 7))


def shift(value, axis, step):
    n = SIZE[axis]
    return lax.ppermute(value, axis, [(i, (i + step) % n) for i in range(n)])


def pick(value, index, axis=0):
    return lax.dynamic_index_in_dim(value, index, axis, keepdims=False)


def contract_tokens(left, right):
    return lax.dot_general(left, right, (((0,), (0,)), ((), ())), preferred_element_type=jnp.float32)


def per_device(act_a, act_b):
    rows, own_units = act_a.shape
    shard, units = act_b.shape
    band = units // (NZ * NY * NC)
    total = rows * NZ * NY * NC
    per_z = units // NZ
    z, y, c, x = (lax.axis_index(n) for n in ("z", "y", "c", "x"))

    quarters = act_a.reshape(NX, shard, own_units)
    turned = jnp.concatenate([pick(quarters, (x + s) % NX) for s in (0, -1, 1, 2)], axis=0)

    columns = [jnp.concatenate([act_b[:, q * per_z:(q + 1) * per_z] for q in zs], axis=1) for zs in CHUNKS]
    gathered = []
    for k, block in enumerate(columns):
        if k >= 2:
            block, _ = lax.optimization_barrier((block, gathered[k - 1][1:3]))
        left = shift(block, "x", 1)
        right = shift(block, "x", -1)
        half = shard // 2
        far_low = shift(left[:half], "x", 1)
        far_high = shift(right[half:], "x", -1)
        gathered.append((block, left, right, far_low, far_high))

    wide_a = act_a.astype(jnp.float32)
    wide_b = act_b.astype(jnp.float32)
    stats = jnp.concatenate(
        [jnp.sum(wide_a, axis=0), jnp.sum(wide_a * wide_a, axis=0), jnp.sum(wide_b, axis=0), jnp.sum(wide_b * wide_b, axis=0)]
    )
    for axis in TOK:
        stats = lax.psum(stats, axis)
    a_sum, a_square, b_sum, b_square = jnp.split(stats, [own_units, 2 * own_units, 2 * own_units + units])
    start = ((z * NY + y) * NC + c) * band
    own_b = jnp.stack([lax.dynamic_slice_in_dim(b_sum, start, band), lax.dynamic_slice_in_dim(b_square, start, band)])
    own_b = own_b + shift(own_b, "x", 1) + shift(own_b, "x", -1) + shift(own_b, "x", 2)

    shares = None
    for zs, blocks in zip(CHUNKS, gathered):
        product = contract_tokens(jnp.concatenate(blocks, axis=0), turned)
        product = product.reshape(len(zs), NY, NC, band, own_units)
        other = shift(pick(product, 1 - c, 2), "c", 1)
        mine = pick(product, c, 2)
        parts = {s: pick(mine, (y + s) % NY, 1) + pick(other, (y + s) % NY, 1) for s in (0, 1, -1, 2)}
        summed = parts[0]
        for s in (1, -1, 2):
            summed = summed + shift(parts[s], "y", s)
        got = []
        for s in (1, -1, 2, -2, 3, -3, 4):
            pairs = [((q - s) % NZ, q) for q in zs]
            send = jnp.where((z + s) % NZ == zs[0], summed[0], summed[-1])
            got.append(lax.ppermute(send, "z", pairs))
        hit = functools.reduce(jnp.logical_or, [z == q for q in zs])
        total_here = jnp.where(z == zs[0], summed[0], summed[-1])
        for g in got:
            total_here = total_here + g
        shares = jnp.where(hit, total_here, 0.0 if shares is None else shares)

    mean_a = a_sum / total
    var_a = a_square / total - mean_a * mean_a
    mean_b = own_b[0] / total
    var_b = own_b[1] / total - mean_b * mean_b
    centered = shares / total - mean_b[:, None] * mean_a[None, :]
    return centered / (jnp.sqrt(var_b + 1e-05)[:, None] * jnp.sqrt(var_a + 1e-05)[None, :])


def solution(mesh):
    torus = Mesh(mesh.devices.reshape(NZ, NY, NC, NX), ("z", "y", "c", "x"))
    return jax.shard_map(
        per_device,
        mesh=torus,
        in_specs=(P(TOK, "x"), P(("z", "y", "c", "x"), None)),
        out_specs=P(TOK, "x"),
        check_vma=False,
    )
```

```python
import jax
import jax.numpy as jnp
from jax import lax
from jax.sharding import Mesh
from jax.sharding import PartitionSpec as P

NZ, NY, NC, NX = 8, 4, 2, 4
SIZE = {"z": NZ, "y": NY, "c": NC, "x": NX}
TOK = ("z", "y", "c")
CHUNKS = ((4,), (3, -3), (2, -2), (1, -1), (0,))


def shift(value, axis, step):
    n = SIZE[axis]
    return lax.ppermute(value, axis, [(i, (i + step) % n) for i in range(n)])


def pick(value, index, axis=0):
    return lax.dynamic_index_in_dim(value, index, axis, keepdims=False)


def after(value, token):
    return value if token is None else lax.optimization_barrier((value, token))[0]


def contract_tokens(left, right):
    return lax.dot_general(left, right, (((0,), (0,)), ((), ())), preferred_element_type=jnp.float32)


def per_device(act_a, act_b):
    rows, own_units = act_a.shape
    units = act_b.shape[1]
    band = units // (NZ * NY * NC)
    total = rows * NZ * NY * NC
    per_z = units // NZ
    z, y, c = (lax.axis_index(n) for n in TOK)

    blocks = []
    for steps in CHUNKS:
        cut = [lax.dynamic_slice_in_dim(act_b, ((z + d) % NZ) * per_z, per_z, 1) for d in steps]
        blocks.append(cut[0] if len(cut) == 1 else jnp.concatenate(cut, axis=1))

    wide_a = act_a.astype(jnp.float32)
    wide_b = act_b.astype(jnp.float32)
    stats = jnp.concatenate(
        [jnp.sum(wide_a, axis=0), jnp.sum(wide_a * wide_a, axis=0), jnp.sum(wide_b, axis=0), jnp.sum(wide_b * wide_b, axis=0)]
    )
    for axis, steps in (("c", (1,)), ("y", (2, 1)), ("z", (4, 2, 1))):
        for step in steps:
            stats = stats + shift(stats, axis, step)

    gathered = []
    for k, block in enumerate(blocks):
        block = after(block, gathered[k - 2] if k >= 2 else None)
        gathered.append(lax.all_gather(block, "x", axis=0, tiled=True))

    result, summed, parts = None, None, None
    for k, steps in enumerate(CHUNKS):
        n = len(steps)
        tokens = after(gathered[k], stats if k == 0 else tuple(parts.values()))
        product = contract_tokens(tokens, act_a)
        product = after(product, summed)
        product = product.reshape(n, NY, NC, band, own_units)
        other = shift(pick(product, 1 - c, 2), "c", 1)
        mine = pick(product, c, 2)
        parts = {s: pick(mine, (y + s) % NY, 1) + pick(other, (y + s) % NY, 1) for s in (0, 1, -1, 2)}
        summed = parts[0]
        for s in (1, -1, 2):
            summed = summed + shift(parts[s], "y", s)
        for i, d in enumerate(steps):
            got = summed[i] if d == 0 else shift(summed[i], "z", d)
            result = got if result is None else result + got
        if k == 1:
            start = ((z * NY + y) * NC + c) * band
            b_sums = after(stats[2 * own_units:], summed).reshape(2, units)
            own_b = lax.dynamic_slice_in_dim(b_sums, start, band, 1)
            own_b = own_b + shift(own_b, "x", 2)
            own_b = own_b + shift(own_b, "x", 1)

    mean_a = stats[:own_units] / total
    var_a = stats[own_units:2 * own_units] / total - mean_a * mean_a
    mean_b = own_b[0] / total
    var_b = own_b[1] / total - mean_b * mean_b
    centered = result / total - mean_b[:, None] * mean_a[None, :]
    return centered / (jnp.sqrt(var_b + 1e-05)[:, None] * jnp.sqrt(var_a + 1e-05)[None, :])


def solution(mesh):
    torus = Mesh(mesh.devices.reshape(NZ, NY, NC, NX), ("z", "y", "c", "x"))
    return jax.shard_map(
        per_device,
        mesh=torus,
        in_specs=(P(TOK, "x"), P(("z", "y", "c", "x"), None)),
        out_specs=P(TOK, "x"),
        check_vma=False,
    )
```

```python
import jax
import jax.numpy as jnp
from jax import lax
from jax.sharding import Mesh
from jax.sharding import PartitionSpec as P


NZ, NY, NC, NX = 8, 4, 2, 4
SIZE = {"z": NZ, "y": NY, "c": NC, "x": NX}
TOK = ("z", "y", "c")
CHUNKS = ((4,), (3, -3), (2, -2), (1, -1), (0,))
PAIR_B = [(0, 1), (1, 0), (2, 3), (3, 2)]
PAIR_A = [(0, 3), (3, 0), (1, 2), (2, 1)]


def shift(value, axis, step):
    n = SIZE[axis]
    return lax.ppermute(value, axis, [(i, (i + step) % n) for i in range(n)])


def pick(value, index, axis=0):
    return lax.dynamic_index_in_dim(value, index, axis, keepdims=False)


def after(value, token):
    return value if token is None else lax.optimization_barrier((value, token))[0]


def contract_tokens(left, right):
    return lax.dot_general(left, right, (((0,), (0,)), ((), ())), preferred_element_type=jnp.float32)


def totals(value):
    wide = value.astype(jnp.float32)
    return jnp.sum(wide, axis=0), jnp.sum(wide * wide, axis=0)


def body(act_a, act_b):
    rows, own = act_a.shape
    shard, units = act_b.shape
    band = units // (NZ * NY * NC)
    total = rows * NZ * NY * NC
    half = rows // 2
    pair_total = total // 2
    per_z = units // NZ
    z, y, c, x = (lax.axis_index(n) for n in ("z", "y", "c", "x"))
    pair = x // 2

    my_a = lax.dynamic_slice_in_dim(act_a, pair * half, half, 0)
    other_a = lax.dynamic_slice_in_dim(act_a, (1 - pair) * half, half, 0)
    b_sum, b_square = totals(act_b)
    b_stats = jnp.stack([b_sum, b_square])
    b_stats = b_stats + lax.ppermute(b_stats, "x", PAIR_B)
    blocks, others = [], []
    for k, steps in enumerate(CHUNKS):
        cut = [lax.dynamic_slice_in_dim(act_b, ((z + d) % NZ) * per_z, per_z, 1) for d in steps]
        blocks.append(cut[0] if len(cut) == 1 else jnp.concatenate(cut, axis=1))
        others.append(lax.ppermute(blocks[k], "x", PAIR_B))
    wide = jnp.concatenate([my_a, lax.ppermute(other_a, "x", PAIR_A)], axis=1)
    (my_sum, my_square), (ot_sum, ot_square) = totals(my_a), totals(other_a)
    a_stats = jnp.stack([my_sum, ot_sum, my_square + ot_square])
    a_other = lax.ppermute(a_stats, "x", PAIR_A)
    a_core = jnp.concatenate([a_stats[0], a_other[1]])
    a_all = jnp.concatenate([a_stats[0] + a_stats[1], a_other[0] + a_other[1]])
    a_square = jnp.concatenate([a_stats[2], a_other[2]])

    stats = jnp.concatenate([a_core, a_all, a_square, b_stats[0], b_stats[1]])
    count = 0
    for axis, hops in (("c", (1,)), ("y", (2, 1)), ("z", (4, 2, 1))):
        for hop in hops:
            stats = stats + shift(stats, axis, hop)
            count += 1
    two = 2 * own
    a_pair, a_all, a_square = stats[:two], stats[two:2 * two], stats[2 * two:3 * two]
    b_pair, b_square = stats[3 * two:3 * two + units], stats[3 * two + units:]

    mean_a = a_all / total
    var_a = a_square / total - mean_a * mean_a
    scale_a = 0.25 * lax.rsqrt(jnp.maximum(var_a, 1e-6 * (a_square / total)) + 1e-05)
    mid_b = b_pair / pair_total
    power_b = b_square / pair_total
    scale_b = lax.rsqrt(jnp.maximum(power_b - mid_b * mid_b, 1e-6 * power_b) + 1e-05)
    lean_a = a_core - half * mean_a
    b_rows = jnp.stack([b_stats[0], mid_b, scale_b]).reshape(3, NZ, per_z)

    low = (x % 2) * shard
    high = (1 - x % 2) * shard
    wide_own = lax.dynamic_slice_in_dim(wide, low, shard, 0)
    wide_far = lax.dynamic_slice_in_dim(wide, high, shard, 0)

    def product_of(k, token):
        steps = CHUNKS[k]
        far = after(others[k], token)
        raw = contract_tokens(blocks[k], wide_own) + contract_tokens(far, wide_far)
        rows_k = jnp.concatenate([pick(b_rows, (z + d) % NZ, 1) for d in steps], axis=1)
        core_b, mean_k, scale_k = rows_k[0], rows_k[1], rows_k[2]
        product = raw - core_b[:, None] * mean_a[None, :] - mean_k[:, None] * lean_a[None, :]
        product = product * scale_k[:, None] * scale_a[None, :]
        product = product.reshape(len(steps), NY, NC, band, two)
        send = pick(product, 1 - c, 2)
        return pick(product, c, 2), send, shift(send, "c", 1)

    def parts_of(mine, other):
        out = [pick(mine, (y + s) % NY, 1) + pick(other, (y + s) % NY, 1) for s in (0, 1, -1, 2)]
        return [out[0]] + [v.astype(jnp.float16) for v in out[1:]]

    count = len(CHUNKS)
    queue = [product_of(0, None), product_of(1, None)]
    parts = parts_of(queue[0][0], queue[0][2])
    result = None
    for k, steps in enumerate(CHUNKS):
        moved = [shift(v, "y", s) for s, v in zip((1, -1, 2), parts[1:])]
        base = parts[0]
        if k + 1 < count:
            mine, _, other = queue[k + 1]
            if k + 2 < count:
                queue.append(product_of(k + 2, tuple(parts)))
                other = after(other, queue[k + 2][1])
            parts = parts_of(mine, other)
            moved = after(moved, tuple(parts))
        summed = base
        for v in moved:
            summed = summed + v.astype(jnp.float32)
        if k + 1 < count:
            parts = after(parts, summed)
        for i, d in enumerate(steps):
            got = summed[i] if d == 0 else shift(summed[i], "z", d)
            result = got if result is None else result + got

    start = ((z * NY + y) * NC + c) * band
    own_b = [lax.dynamic_slice_in_dim(v, start, band) for v in (b_pair, b_square, mid_b, scale_b)]
    pair_b = jnp.stack(own_b[:2])
    pair_b = pair_b + lax.ppermute(pair_b, "x", PAIR_A)
    spread = result / (own_b[3][:, None] * scale_a[None, :])
    spread = spread + own_b[2][:, None] * (a_pair - pair_total * mean_a)[None, :]
    centered = spread[:, :own] + lax.ppermute(spread[:, own:], "x", PAIR_A)
    mean_b = pair_b[0] / total
    var_b = pair_b[1] / total - mean_b * mean_b
    deviation = jnp.sqrt(var_b + 1e-05)[:, None] * jnp.sqrt(var_a[:own] + 1e-05)[None, :]
    return centered / total / deviation


def solution(mesh):
    torus = Mesh(mesh.devices.reshape(NZ, NY, NC, NX), ("z", "y", "c", "x"))
    return jax.shard_map(
        body,
        mesh=torus,
        in_specs=(P(TOK, "x"), P(("z", "y", "c", "x"), None)),
        out_specs=P(TOK, "x"),
        check_vma=False,
    )
```

```python
import jax
import jax.numpy as jnp
from jax import lax
from jax.sharding import Mesh
from jax.sharding import PartitionSpec as P


NZ, NY, NC, NX = 8, 4, 2, 4
SIZE = {"z": NZ, "y": NY, "c": NC, "x": NX}
TOK = ("z", "y", "c")
CHUNKS = ((4,), (3, -3), (2, -2), (1, -1), (0,))
PAIR_B = [(0, 1), (1, 0), (2, 3), (3, 2)]
PAIR_A = [(0, 3), (3, 0), (1, 2), (2, 1)]


def shift(value, axis, step):
    n = SIZE[axis]
    return lax.ppermute(value, axis, [(i, (i + step) % n) for i in range(n)])


def pick(value, index, axis=0):
    return lax.dynamic_index_in_dim(value, index, axis, keepdims=False)


def after(value, token):
    return value if token is None else lax.optimization_barrier((value, token))[0]


def contract_tokens(left, right):
    return lax.dot_general(left, right, (((0,), (0,)), ((), ())), preferred_element_type=jnp.float32)


def rolled(value, offset):
    width = value.shape[1]
    return lax.dynamic_slice_in_dim(jnp.concatenate([value, value], axis=1), offset, width, 1)


def totals(value):
    wide = value.astype(jnp.float32)
    return jnp.sum(wide, axis=0), jnp.sum(wide * wide, axis=0)


def body(act_a, act_b):
    rows, own = act_a.shape
    shard, units = act_b.shape
    band = units // (NZ * NY * NC)
    total = rows * NZ * NY * NC
    half = rows // 2
    per_z = units // NZ
    z, y, c, x = (lax.axis_index(n) for n in ("z", "y", "c", "x"))
    pair = x // 2

    other_a = lax.optimization_barrier(lax.dynamic_slice_in_dim(act_a, (1 - pair) * half, half, 0))
    moved_a = lax.ppermute(other_a, "x", PAIR_A)
    b_core = rolled(jnp.stack(totals(act_b)), z * per_z)
    b_core = b_core + lax.ppermute(b_core, "x", PAIR_B)
    blocks, others = [], []
    for k, steps in enumerate(CHUNKS):
        cut = [lax.dynamic_slice_in_dim(act_b, ((z + d) % NZ) * per_z, per_z, 1) for d in steps]
        blocks.append(cut[0] if len(cut) == 1 else jnp.concatenate(cut, axis=1))
        others.append(lax.ppermute(blocks[k], "x", PAIR_B))
    my_a = lax.dynamic_slice_in_dim(after(act_a, other_a), pair * half, half, 0)
    my_core, ot_core = jnp.stack(totals(my_a)), jnp.stack(totals(other_a))

    stats = jnp.concatenate([b_core, my_core, ot_core], axis=1)
    count = 0
    for axis, hops in (("c", (1,)), ("y", (2, 1))):
        for hop in hops:
            stats = stats + shift(stats, axis, hop)
            count += 1
    group = half * NY * NC
    two = 2 * own
    ours = jnp.concatenate([stats[:, units + own:], ot_core[:1]], axis=0)
    theirs = lax.ppermute(ours, "x", PAIR_A)
    both = jnp.concatenate([stats[:, units:units + own], theirs[:2]], axis=1) / group
    a_core = jnp.concatenate([my_core[:1], theirs[2:]], axis=1)
    mean_a, power_a = both[:1], both[1:]
    mean_b, power_b = stats[:1, :units] / group, stats[1:, :units] / group
    spread_a = jnp.sqrt(jnp.maximum(power_a - mean_a * mean_a, 1e-6 * power_a) + 1e-05)
    spread_b = jnp.sqrt(jnp.maximum(power_b - mean_b * mean_b, 1e-6 * power_b) + 1e-05)
    scale_a, scale_b = 0.25 / spread_a, 1.0 / spread_b
    lean_a = a_core - half * mean_a
    undo_a = 4.0 * spread_a

    wide = jnp.concatenate([my_a, moved_a], axis=1)
    wide_own = lax.dynamic_slice_in_dim(wide, (x % 2) * shard, shard, 0)
    wide_far = lax.dynamic_slice_in_dim(wide, (1 - x % 2) * shard, shard, 0)

    def product_of(k, token):
        steps = CHUNKS[k]
        far = after(others[k], token)
        raw = contract_tokens(blocks[k], wide_own) + contract_tokens(far, wide_far)
        core_b, mean_k, scale_k = (
            jnp.concatenate([v[0, (d % NZ) * per_z:(d % NZ + 1) * per_z] for d in steps])[:, None] for v in (b_core, mean_b, scale_b)
        )
        product = (raw - core_b * mean_a - mean_k * lean_a) * scale_k * scale_a
        product = product.reshape(len(steps), NY, NC, band, two)
        send = pick(product, 1 - c, 2)
        return pick(product, c, 2), send, shift(send, "c", 1)

    def parts_of(mine, other):
        out = [pick(mine, (y + s) % NY, 1) + pick(other, (y + s) % NY, 1) for s in (0, 1, -1, 2)]
        return [out[0]] + [v.astype(jnp.float16) for v in out[1:]]

    count = len(CHUNKS)
    queue = [product_of(0, None), product_of(1, None)]
    parts = parts_of(queue[0][0], queue[0][2])
    result = None
    late, spread_b, mean_b = after((stats, spread_b, mean_b), tuple(parts))
    undo_b = jnp.concatenate([spread_b, group * mean_b], axis=0)
    rest = jnp.concatenate([rolled(late[:, :units], (NZ - z) % NZ * per_z), late[:, units:units + own] + late[:, units + own:]], axis=1)
    for k, steps in enumerate(CHUNKS):
        moved = [shift(v, "y", s) for s, v in zip((1, -1, 2), parts[1:])]
        base = parts[0]
        if k + 1 < count:
            mine, _, other = queue[k + 1]
            if k + 2 < count:
                queue.append(product_of(k + 2, tuple(parts)))
                other = after(other, queue[k + 2][1])
            else:
                other = after(other, tuple(parts))
            parts = parts_of(mine, other)
            moved = after(moved, tuple(parts))
        if 1 <= k <= 3:
            rest = rest + after(moving, tuple(parts))
        summed = base
        for v in moved:
            summed = summed + v.astype(jnp.float32)
        if k + 2 < count:
            parts = after(parts, summed)
        rows = jnp.stack([lax.dynamic_slice_in_dim(undo_b, d % NZ * per_z + (y * NC + c) * band, band, 1) for d in steps], axis=1)
        summed = summed * rows[0][:, :, None] * undo_a + rows[1][:, :, None] * mean_a
        if k < 3:
            moving = shift(after(rest, tuple(parts)), "z", (4, 2, 1)[k])
        for i, d in enumerate(steps):
            got = summed[i] if d == 0 else shift(summed[i], "z", d)
            result = got if result is None else result + got

    start = ((z * NY + y) * NC + c) * band
    b_own = lax.dynamic_slice_in_dim(rest, start, band, 1)
    b_own = b_own + lax.ppermute(b_own, "x", PAIR_A)
    raw = result[:, :own] + lax.ppermute(result[:, own:], "x", PAIR_A)
    mean_a = rest[0, units:] / total
    var_a = rest[1, units:] / total - mean_a * mean_a
    mean_b = b_own[0] / total
    var_b = b_own[1] / total - mean_b * mean_b
    centered = raw / total - mean_b[:, None] * mean_a[None, :]
    return centered / (jnp.sqrt(var_b + 1e-05)[:, None] * jnp.sqrt(var_a + 1e-05)[None, :])


def solution(mesh):
    torus = Mesh(mesh.devices.reshape(NZ, NY, NC, NX), ("z", "y", "c", "x"))
    return jax.shard_map(
        body,
        mesh=torus,
        in_specs=(P(TOK, "x"), P(("z", "y", "c", "x"), None)),
        out_specs=P(TOK, "x"),
        check_vma=False,
    )
```

```python
import jax
import jax.numpy as jnp
from jax import lax
from jax.sharding import Mesh
from jax.sharding import PartitionSpec as P


NZ, NY, NC, NX = 8, 4, 2, 4
SIZE = {"z": NZ, "y": NY, "c": NC, "x": NX}
TOK = ("z", "y", "c")
CHUNKS = ((4,), (3, -3), (2, -2), (1, -1), (0,))
PAIR_B = [(0, 1), (1, 0), (2, 3), (3, 2)]
PAIR_A = [(0, 3), (3, 0), (1, 2), (2, 1)]


def shift(value, axis, step):
    n = SIZE[axis]
    return lax.ppermute(value, axis, [(i, (i + step) % n) for i in range(n)])


def pick(value, index, axis=0):
    return lax.dynamic_index_in_dim(value, index, axis, keepdims=False)


def after(value, token):
    return value if token is None else lax.optimization_barrier((value, token))[0]


def contract_tokens(left, right):
    return lax.dot_general(left, right, (((0,), (0,)), ((), ())), preferred_element_type=jnp.float32)


def rolled(value, offset):
    width = value.shape[1]
    return lax.dynamic_slice_in_dim(jnp.concatenate([value, value], axis=1), offset, width, 1)


def totals(value):
    wide = value.astype(jnp.float32)
    return jnp.sum(wide, axis=0), jnp.sum(wide * wide, axis=0)


def body(act_a, act_b):
    rows, own = act_a.shape
    shard, units = act_b.shape
    band = units // (NZ * NY * NC)
    total = rows * NZ * NY * NC
    half = rows // 2
    per_z = units // NZ
    z, y, c, x = (lax.axis_index(n) for n in ("z", "y", "c", "x"))
    pair = x // 2

    other_a = lax.optimization_barrier(lax.dynamic_slice_in_dim(act_a, (1 - pair) * half, half, 0))
    moved_a = lax.ppermute(other_a, "x", PAIR_A)
    b_core = rolled(jnp.stack(totals(act_b)), z * per_z)
    b_core = b_core + lax.ppermute(b_core, "x", PAIR_B)
    blocks, others = [], []
    for k, steps in enumerate(CHUNKS):
        cut = [lax.dynamic_slice_in_dim(act_b, ((z + d) % NZ) * per_z, per_z, 1) for d in steps]
        blocks.append(cut[0] if len(cut) == 1 else jnp.concatenate(cut, axis=1))
        others.append(lax.ppermute(blocks[k], "x", PAIR_B))
    my_a = lax.dynamic_slice_in_dim(after(act_a, other_a), pair * half, half, 0)
    my_core, ot_core = jnp.stack(totals(my_a)), jnp.stack(totals(other_a))

    stats = jnp.concatenate([b_core, my_core, ot_core], axis=1)
    count = 0
    for axis, hops in (("c", (1,)), ("y", (2, 1))):
        for hop in hops:
            stats = stats + shift(stats, axis, hop)
            count += 1
    group = half * NY * NC
    two = 2 * own
    ours = jnp.concatenate([stats[:, units + own:], ot_core[:1]], axis=0)
    theirs = lax.ppermute(ours, "x", PAIR_A)
    both = jnp.concatenate([stats[:, units:units + own], theirs[:2]], axis=1) / group
    a_core = jnp.concatenate([my_core[:1], theirs[2:]], axis=1)
    mean_a, power_a = both[:1], both[1:]
    mean_b, power_b = stats[:1, :units] / group, stats[1:, :units] / group
    spread_a = jnp.sqrt(jnp.maximum(power_a - mean_a * mean_a, 1e-6 * power_a) + 1e-05)
    spread_b = jnp.sqrt(jnp.maximum(power_b - mean_b * mean_b, 1e-6 * power_b) + 1e-05)
    scale_a, scale_b = 0.25 / spread_a, 1.0 / spread_b
    lean_a = a_core - half * mean_a
    undo_a = 4.0 * spread_a

    wide = jnp.concatenate([my_a, moved_a], axis=1)
    wide_own = lax.dynamic_slice_in_dim(wide, (x % 2) * shard, shard, 0)
    wide_far = lax.dynamic_slice_in_dim(wide, (1 - x % 2) * shard, shard, 0)

    def product_of(k, token):
        steps = CHUNKS[k]
        far = after(others[k], token)
        raw = contract_tokens(blocks[k], wide_own) + contract_tokens(far, wide_far)
        core_b, mean_k, scale_k = (
            jnp.concatenate([v[0, (d % NZ) * per_z:(d % NZ + 1) * per_z] for d in steps])[:, None] for v in (b_core, mean_b, scale_b)
        )
        product = (raw - core_b * mean_a - mean_k * lean_a) * scale_k * scale_a
        product = product.reshape(len(steps), NY, NC, band, two)
        send = pick(product, 1 - c, 2)
        return pick(product, c, 2), send, shift(send, "c", 1)

    def parts_of(mine, other):
        out = [pick(mine, (y + s) % NY, 1) + pick(other, (y + s) % NY, 1) for s in (0, 1, -1, 2)]
        return [out[0]] + [v.astype(jnp.float16) for v in out[1:]]

    count = len(CHUNKS)
    queue = [product_of(0, None), product_of(1, None)]
    parts = parts_of(queue[0][0], queue[0][2])
    late, spread_b, mean_b = after((stats, spread_b, mean_b), tuple(parts))
    undo_b = jnp.concatenate([spread_b, group * mean_b, late[:, :units]], axis=0)
    late_a = late[:, units:units + own] + late[:, units + own:]
    late_a = jnp.concatenate([late_a[:1], late_a[1:]], axis=1)
    up, down = None, None
    for k, steps in enumerate(CHUNKS):
        moved = [shift(v, "y", s) for s, v in zip((1, -1, 2), parts[1:])]
        base = parts[0]
        if k + 1 < count:
            mine, _, other = queue[k + 1]
            if k + 2 < count:
                queue.append(product_of(k + 2, tuple(parts)))
                other = after(other, queue[k + 2][1])
            else:
                other = after(other, tuple(parts))
            parts = parts_of(mine, other)
            moved = after(moved, tuple(parts))
        else:
            moved = after(moved, tuple(sent))
        summed = base
        for v in moved:
            summed = summed + v.astype(jnp.float32)
        if k + 2 < count:
            parts = after(parts, summed)
        rows = jnp.stack([lax.dynamic_slice_in_dim(undo_b, d % NZ * per_z + (y * NC + c) * band, band, 1) for d in steps], axis=1)
        summed = summed * rows[0][:, :, None] * undo_a + rows[1][:, :, None] * mean_a
        sent = []
        for i, d in enumerate(steps):
            counts = jnp.pad(rows[2:4, i], ((0, 5), (own, two - own - band)))
            piece = jnp.concatenate([summed[i], late_a, counts], axis=0)
            if d > 0:
                sent.append(piece if up is None else piece + up)
                up = shift(sent[-1], "z", 1)
            elif d < 0:
                sent.append(piece if down is None else piece + down)
                down = shift(sent[-1], "z", -1)
            else:
                result = piece + up + down

    partner = lax.ppermute(result[:, own:], "x", PAIR_A)
    raw = result[:band, :own] + partner[:band]
    mean_a = result[band, :own] / total
    var_a = result[band, own:] / total - mean_a * mean_a
    b_own = result[band + 1:band + 3, own:own + band] + partner[band + 1:band + 3, :band]
    mean_b = b_own[0] / total
    var_b = b_own[1] / total - mean_b * mean_b
    centered = raw / total - mean_b[:, None] * mean_a[None, :]
    return centered / (jnp.sqrt(var_b + 1e-05)[:, None] * jnp.sqrt(var_a + 1e-05)[None, :])


def solution(mesh):
    torus = Mesh(mesh.devices.reshape(NZ, NY, NC, NX), ("z", "y", "c", "x"))
    return jax.shard_map(
        body,
        mesh=torus,
        in_specs=(P(TOK, "x"), P(("z", "y", "c", "x"), None)),
        out_specs=P(TOK, "x"),
        check_vma=False,
    )
```

```python
import jax
import jax.numpy as jnp
from jax import lax
from jax.sharding import Mesh
from jax.sharding import PartitionSpec as P


NZ, NY, NC, NX = 8, 4, 2, 4
SIZE = {"z": NZ, "y": NY, "c": NC, "x": NX}
TOK = ("z", "y", "c")
CHUNKS = ((4, 0), (3, -3), (2, -2), (1, -1))
PAIR_B = [(0, 1), (1, 0), (2, 3), (3, 2)]
PAIR_A = [(0, 3), (3, 0), (1, 2), (2, 1)]


def shift(value, axis, step):
    n = SIZE[axis]
    return lax.ppermute(value, axis, [(i, (i + step) % n) for i in range(n)])


def pick(value, index, axis=0):
    return lax.dynamic_index_in_dim(value, index, axis, keepdims=False)


def after(value, token):
    return value if token is None else lax.optimization_barrier((value, token))[0]


def contract_tokens(left, right):
    return lax.dot_general(left, right, (((0,), (0,)), ((), ())), preferred_element_type=jnp.float32)


def rolled(value, offset):
    width = value.shape[1]
    return lax.dynamic_slice_in_dim(jnp.concatenate([value, value], axis=1), offset, width, 1)


def totals(value):
    wide = value.astype(jnp.float32)
    return jnp.sum(wide, axis=0), jnp.sum(wide * wide, axis=0)


def body(act_a, act_b):
    rows, own = act_a.shape
    shard, units = act_b.shape
    band = units // (NZ * NY * NC)
    total = rows * NZ * NY * NC
    half = rows // 2
    per_z = units // NZ
    z, y, c, x = (lax.axis_index(n) for n in ("z", "y", "c", "x"))
    pair = x // 2

    other_a = lax.optimization_barrier(lax.dynamic_slice_in_dim(act_a, (1 - pair) * half, half, 0))
    moved_a = lax.ppermute(other_a, "x", PAIR_A)
    b_core = rolled(jnp.stack(totals(act_b)), z * per_z)
    b_core = b_core + lax.ppermute(b_core, "x", PAIR_B)
    blocks, others = [], []
    for k, steps in enumerate(CHUNKS):
        cut = [lax.dynamic_slice_in_dim(act_b, ((z + d) % NZ) * per_z, per_z, 1) for d in steps]
        blocks.append(cut[0] if len(cut) == 1 else jnp.concatenate(cut, axis=1))
        others.append(lax.ppermute(blocks[k], "x", PAIR_B))
    my_a = lax.dynamic_slice_in_dim(after(act_a, other_a), pair * half, half, 0)
    my_core, ot_core = jnp.stack(totals(my_a)), jnp.stack(totals(other_a))

    stats = jnp.concatenate([b_core, my_core, ot_core], axis=1)
    count = 0
    for axis, hops in (("c", (1,)), ("y", (2, 1))):
        for hop in hops:
            stats = stats + shift(stats, axis, hop)
            count += 1
    group = half * NY * NC
    two = 2 * own
    ours = jnp.concatenate([stats[:, units + own:], ot_core[:1]], axis=0)
    theirs = lax.ppermute(ours, "x", PAIR_A)
    both = jnp.concatenate([stats[:, units:units + own], theirs[:2]], axis=1) / group
    a_core = jnp.concatenate([my_core[:1], theirs[2:]], axis=1)
    mean_a, power_a = both[:1], both[1:]
    mean_b, power_b = stats[:1, :units] / group, stats[1:, :units] / group
    spread_a = jnp.sqrt(jnp.maximum(power_a - mean_a * mean_a, 1e-6 * power_a) + 1e-05)
    spread_b = jnp.sqrt(jnp.maximum(power_b - mean_b * mean_b, 1e-6 * power_b) + 1e-05)
    scale_a, scale_b = 0.25 / spread_a, 1.0 / spread_b
    lean_a = a_core - half * mean_a
    undo_a = 4.0 * spread_a

    wide = jnp.concatenate([my_a, moved_a], axis=1)
    wide_own = lax.dynamic_slice_in_dim(wide, (x % 2) * shard, shard, 0)
    wide_far = lax.dynamic_slice_in_dim(wide, (1 - x % 2) * shard, shard, 0)

    def product_of(k, token):
        steps = CHUNKS[k]
        far = after(others[k], token)
        raw = contract_tokens(blocks[k], wide_own) + contract_tokens(far, wide_far)
        core_b, mean_k, scale_k = (
            jnp.concatenate([v[0, (d % NZ) * per_z:(d % NZ + 1) * per_z] for d in steps])[:, None] for v in (b_core, mean_b, scale_b)
        )
        product = (raw - core_b * mean_a - mean_k * lean_a) * scale_k * scale_a
        product = product.reshape(len(steps), NY, NC, band, two)
        send = pick(product, 1 - c, 2)
        return pick(product, c, 2), send, shift(send, "c", 1)

    def parts_of(mine, other):
        out = [pick(mine, (y + s) % NY, 1) + pick(other, (y + s) % NY, 1) for s in (0, 1, -1, 2)]
        return [out[0]] + [v.astype(jnp.float16) for v in out[1:]]

    count = len(CHUNKS)
    queue = [product_of(0, None), product_of(1, None)]
    parts = parts_of(queue[0][0], queue[0][2])
    late, spread_b, mean_b = after((stats, spread_b, mean_b), tuple(parts))
    undo_b = jnp.concatenate([spread_b, group * mean_b, late[:, :units]], axis=0)
    late_a = late[:, units:units + own] + late[:, units + own:]
    late_a = jnp.concatenate([late_a[:1], late_a[1:]], axis=1)
    up, down = None, None
    for k, steps in enumerate(CHUNKS):
        moved = [shift(v, "y", s) for s, v in zip((1, -1, 2), parts[1:])]
        base = parts[0]
        if k + 1 < count:
            mine, _, other = queue[k + 1]
            if k + 2 < count:
                queue.append(product_of(k + 2, tuple(parts)))
                other = after(other, queue[k + 2][1])
            else:
                other = after(other, tuple(parts))
            parts = parts_of(mine, other)
            moved = after(moved, tuple(parts))
        else:
            moved = after(moved, tuple(sent))
        summed = base
        for v in moved:
            summed = summed + v.astype(jnp.float32)
        rows = jnp.stack([lax.dynamic_slice_in_dim(undo_b, d % NZ * per_z + (y * NC + c) * band, band, 1) for d in steps], axis=1)
        whole = summed * rows[0][:, :, None] * undo_a + rows[1][:, :, None] * mean_a
        cuts = [whole[i] for i in range(len(steps))]
        if k + 2 < count:
            parts = after(parts, summed)
        sent = []
        for i, d in enumerate(steps):
            counts = jnp.pad(rows[2:4, i], ((0, 5), (own, two - own - band)))
            piece = jnp.concatenate([cuts[i], late_a, counts], axis=0)
            if d > 0:
                sent.append(piece if up is None else piece + up)
                up = shift(sent[-1], "z", 1)
            elif d < 0:
                sent.append(piece if down is None else piece + down)
                down = shift(sent[-1], "z", -1)
            else:
                stay = piece
    result = stay + up + down

    partner = lax.ppermute(result[:, own:], "x", PAIR_A)
    raw = result[:band, :own] + partner[:band]
    mean_a = result[band, :own] / total
    var_a = result[band, own:] / total - mean_a * mean_a
    b_own = result[band + 1:band + 3, own:own + band] + partner[band + 1:band + 3, :band]
    mean_b = b_own[0] / total
    var_b = b_own[1] / total - mean_b * mean_b
    centered = raw / total - mean_b[:, None] * mean_a[None, :]
    return centered / (jnp.sqrt(var_b + 1e-05)[:, None] * jnp.sqrt(var_a + 1e-05)[None, :])


def solution(mesh):
    torus = Mesh(mesh.devices.reshape(NZ, NY, NC, NX), ("z", "y", "c", "x"))
    return jax.shard_map(
        body,
        mesh=torus,
        in_specs=(P(TOK, "x"), P(("z", "y", "c", "x"), None)),
        out_specs=P(TOK, "x"),
        check_vma=False,
    )
```

```python
import jax
import jax.numpy as jnp
from jax import lax
from jax.sharding import Mesh
from jax.sharding import PartitionSpec as P


NZ, NY, NC, NX = 8, 4, 2, 4
SIZE = {"z": NZ, "y": NY, "c": NC, "x": NX}
TOK = ("z", "y", "c")
CHUNKS = ((4,), (3, -3), (2, -2), (1, -1), (0,))
PAIR_B = [(0, 1), (1, 0), (2, 3), (3, 2)]
PAIR_A = [(0, 3), (3, 0), (1, 2), (2, 1)]


def shift(value, axis, step):
    n = SIZE[axis]
    return lax.ppermute(value, axis, [(i, (i + step) % n) for i in range(n)])


def pick(value, index, axis=0):
    return lax.dynamic_index_in_dim(value, index, axis, keepdims=False)


def after(value, token):
    return value if token is None else lax.optimization_barrier((value, token))[0]


def contract_tokens(left, right):
    return lax.dot_general(left, right, (((0,), (0,)), ((), ())), preferred_element_type=jnp.float32)


def rolled(value, offset):
    width = value.shape[1]
    return lax.dynamic_slice_in_dim(jnp.concatenate([value, value], axis=1), offset, width, 1)


def totals(value):
    wide = value.astype(jnp.float32)
    return jnp.sum(wide, axis=0), jnp.sum(wide * wide, axis=0)


def body(act_a, act_b):
    rows, own = act_a.shape
    shard, units = act_b.shape
    band = units // (NZ * NY * NC)
    total = rows * NZ * NY * NC
    half = rows // 2
    per_z = units // NZ
    z, y, c, x = (lax.axis_index(n) for n in ("z", "y", "c", "x"))
    pair = x // 2

    other_a = lax.optimization_barrier(lax.dynamic_slice_in_dim(act_a, (1 - pair) * half, half, 0))
    moved_a = lax.ppermute(other_a, "x", PAIR_A)
    b_core = rolled(jnp.stack(totals(act_b)), z * per_z)
    b_core = b_core + lax.ppermute(b_core, "x", PAIR_B)
    blocks, others = [], []
    for k, steps in enumerate(CHUNKS):
        cut = [lax.dynamic_slice_in_dim(act_b, ((z + d) % NZ) * per_z, per_z, 1) for d in steps]
        blocks.append(cut[0] if len(cut) == 1 else jnp.concatenate(cut, axis=1))
        others.append(lax.ppermute(blocks[k], "x", PAIR_B))
    my_a = lax.dynamic_slice_in_dim(after(act_a, other_a), pair * half, half, 0)
    my_core, ot_core = jnp.stack(totals(my_a)), jnp.stack(totals(other_a))

    stats = jnp.concatenate([b_core, my_core, ot_core], axis=1)
    count = 0
    for axis, hops in (("c", (1,)), ("y", (2, 1))):
        for hop in hops:
            stats = stats + shift(stats, axis, hop)
            count += 1
    group = half * NY * NC
    two = 2 * own
    ours = jnp.concatenate([stats[:, units + own:], ot_core[:1]], axis=0)
    theirs = lax.ppermute(ours, "x", PAIR_A)
    both = jnp.concatenate([stats[:, units:units + own], theirs[:2]], axis=1) / group
    a_core = jnp.concatenate([my_core[:1], theirs[2:]], axis=1)
    mean_a, power_a = both[:1], both[1:]
    mean_b, power_b = stats[:1, :units] / group, stats[1:, :units] / group
    spread_a = jnp.sqrt(jnp.maximum(power_a - mean_a * mean_a, 1e-6 * power_a) + 1e-05)
    spread_b = jnp.sqrt(jnp.maximum(power_b - mean_b * mean_b, 1e-6 * power_b) + 1e-05)
    scale_a, scale_b = 0.25 / spread_a, 1.0 / spread_b
    lean_a = a_core - half * mean_a
    undo_a = 4.0 * spread_a

    wide = jnp.concatenate([my_a, moved_a], axis=1)
    wide_own = lax.dynamic_slice_in_dim(wide, (x % 2) * shard, shard, 0)
    wide_far = lax.dynamic_slice_in_dim(wide, (1 - x % 2) * shard, shard, 0)

    def product_of(k, token):
        steps = CHUNKS[k]
        far = after(others[k], token)
        raw = contract_tokens(blocks[k], wide_own) + contract_tokens(far, wide_far)
        core_b, mean_k, scale_k = (
            jnp.concatenate([v[0, (d % NZ) * per_z:(d % NZ + 1) * per_z] for d in steps])[:, None] for v in (b_core, mean_b, scale_b)
        )
        product = (raw - core_b * mean_a - mean_k * lean_a) * scale_k * scale_a
        product = product.reshape(len(steps), NY, NC, band, two)
        send = pick(product, 1 - c, 2)
        return pick(product, c, 2), send, shift(send, "c", 1)

    def parts_of(mine, other):
        out = [pick(mine, (y + s) % NY, 1) + pick(other, (y + s) % NY, 1) for s in (0, 1, -1, 2)]
        return [out[0]] + [v.astype(jnp.float16) for v in out[1:]]

    count = len(CHUNKS)
    queue = [product_of(0, None), product_of(1, None)]
    parts = parts_of(queue[0][0], queue[0][2])
    late, spread_b, mean_b = after((stats, spread_b, mean_b), tuple(parts))
    undo_b = jnp.concatenate([spread_b, group * mean_b, late[:, :units]], axis=0)
    late_a = late[:, units:units + own] + late[:, units + own:]
    late_a = jnp.concatenate([late_a[:1], late_a[1:]], axis=1)
    up, down = None, None
    for k, steps in enumerate(CHUNKS):
        moved = [shift(v, "y", s) for s, v in zip((1, -1, 2), parts[1:])]
        base = parts[0]
        if k + 1 < count:
            mine, _, other = queue[k + 1]
            if k + 2 < count:
                queue.append(product_of(k + 2, tuple(parts)))
                other = after(other, queue[k + 2][1])
            else:
                other = after(other, tuple(parts))
            parts = parts_of(mine, other)
            moved = after(moved, tuple(parts))
        else:
            moved = after(moved, tuple(sent))
        summed = base
        for v in moved:
            summed = summed + v.astype(jnp.float32)
        rows = jnp.stack([lax.dynamic_slice_in_dim(undo_b, d % NZ * per_z + (y * NC + c) * band, band, 1) for d in steps], axis=1)
        whole = summed * rows[0][:, :, None] * undo_a + rows[1][:, :, None] * mean_a
        cuts = [whole[i] for i in range(len(steps))]
        sent = []
        for i, d in enumerate(steps):
            counts = jnp.pad(rows[2:4, i], ((0, 5), (own, two - own - band)))
            piece = jnp.concatenate([cuts[i], late_a, counts], axis=0)
            if d > 0:
                sent.append(piece if up is None else piece + up)
                up = shift(sent[-1], "z", 1)
            elif d < 0:
                sent.append(piece if down is None else piece + down)
                down = shift(sent[-1], "z", -1)
            else:
                result = piece + up + down

    partner = lax.ppermute(result[:, own:], "x", PAIR_A)
    raw = result[:band, :own] + partner[:band]
    mean_a = result[band, :own] / total
    var_a = result[band, own:] / total - mean_a * mean_a
    b_own = result[band + 1:band + 3, own:own + band] + partner[band + 1:band + 3, :band]
    mean_b = b_own[0] / total
    var_b = b_own[1] / total - mean_b * mean_b
    centered = raw / total - mean_b[:, None] * mean_a[None, :]
    return centered / (jnp.sqrt(var_b + 1e-05)[:, None] * jnp.sqrt(var_a + 1e-05)[None, :])


def solution(mesh):
    torus = Mesh(mesh.devices.reshape(NZ, NY, NC, NX), ("z", "y", "c", "x"))
    return jax.shard_map(
        body,
        mesh=torus,
        in_specs=(P(TOK, "x"), P(("z", "y", "c", "x"), None)),
        out_specs=P(TOK, "x"),
        check_vma=False,
    )
```
